32 devices in a mesh: dp: 2 (over z, core), tp: 16 (over x, y).
Axes of the slice: x: 4, y: 4, z: 1, core: 2. Of those that a mesh axis runs over, the one named last changes fastest.
The devices are a block of a 4x4x8 slice.
Arguments:
- x: bfloat16 [256, 8192], P('dp'), parts along dimension 0
- w_gate: bfloat16 [8192, 32768], P(None, 'tp')
- w_up: bfloat16 [8192, 32768], P(None, 'tp')
- w_down: bfloat16 [32768, 8192], P('tp')
Outputs:
- output: bfloat16 [256, 8192], P('dp'), parts along dimension 0
There are 2 independent parts. The reference program is written for one: setup_inputs(seed, part) draws one part's arguments, and reference() takes and returns one part's arrays. A program takes and returns all parts, laid end to end along the dimension named above; an argument that names none is the same for every part.
All inputs are finite; a program needn't handle non-finite values.
Results may differ from the reference program's by a relative error of at most 0.016.
Values are sent between devices in bfloat16 or wider.
A program may use at most 768 MiB of HBM per device.

```python
import jax
import jax.numpy as jnp

ROWS = 128
D = 8192
FF = 32768


def setup_inputs(seed: int = 0, part: int = 0) -> dict:
    kx, kg, ku, kd = jax.random.split(jax.random.key(seed), 4)
    drawn = {
        "x": jax.random.normal(jax.random.fold_in(kx, part), (ROWS, D), jnp.float32),
        "w_gate": jax.random.normal(kg, (D, FF), jnp.float32) * D**-0.5,
        "w_up": jax.random.normal(ku, (D, FF), jnp.float32) * D**-0.5,
        "w_down": jax.random.normal(kd, (FF, D), jnp.float32) * FF**-0.5,
    }
    return {k: v.astype(jnp.bfloat16) for k, v in drawn.items()}


def reference(x, w_gate, w_up, w_down):
    gate = jnp.dot(x, w_gate, preferred_element_type=jnp.float32)
    up = jnp.dot(x, w_up, preferred_element_type=jnp.float32)
    hidden = (jax.nn.silu(gate) * up).astype(jnp.bfloat16)
    return jnp.dot(hidden, w_down, preferred_element_type=jnp.float32).astype(jnp.bfloat16)
```

```python
import functools
import math

import jax
import jax.numpy as jnp
from jax import lax
from jax.experimental import pallas as pl
from jax.experimental.pallas import tpu as pltpu
from jax.sharding import PartitionSpec as P

MESH = pl.DeviceIdType.MESH
F32, BF16 = jnp.float32, jnp.bfloat16

KC = 1024
JC = 512
CW = 512
SLOTS = 8
LAG = 3


def kernel(
    side, x_ref, wg_ref, wu_ref, wd_ref, out_ref,
    xs, wgb, wub, wdb, accg, accu, hid, term, termb, r1, f1, red, redb, r2, f2, swp, ybuf,
    x_in, x_out, x_recv, w_in, wd_in, h_out, h_recv, y_out,
    s_r1, s_f1, s_r2, s_f2, s_sw, s_g1, s_g1f, s_g2, s_g2f,
    q_r1, q_f1, q_r2, q_f2, q_sw, q_g1, q_g2,
):
    rows, depth = x_ref.shape
    hw = wg_ref.shape[1] // 2
    cols = out_ref.shape[1] // 2
    nk, nj, nc = depth // KC, hw // JC, cols // CW
    nblk = nk * nj
    ow = CW // 2
    br, qr, qc = rows // side, rows // side // 2, ow // 2

    dp, tp = lax.axis_index("dp"), lax.axis_index("tp")
    h = lax.rem(dp, 2)
    other = 1 - h
    partner = (dp + 1 - 2 * h, tp)
    cx, cy = tp // side, lax.rem(tp, side)

    def near(axis, d):
        if axis == 0:
            return (dp, lax.rem(cx + d + side, side) * side + cy)
        return (dp, cx * side + lax.rem(cy + d + side, side))

    nbr = [[near(axis, 1), near(axis, -1)] for axis in (0, 1)]
    coord = [cx, cy]

    def send(src, dst, s_sem, r_sem, dev):
        return pltpu.make_async_remote_copy(
            src_ref=src, dst_ref=dst, send_sem=s_sem, recv_sem=r_sem, device_id=dev, device_id_type=MESH
        )

    def landed(dst, r_sem):
        pltpu.make_async_remote_copy(
            src_ref=dst, dst_ref=dst, send_sem=s_sw, recv_sem=r_sem, device_id=partner, device_id_type=MESH
        ).wait_recv()

    def left_device(ref, s_sem):
        pltpu.make_async_remote_copy(
            src_ref=ref, dst_ref=ref, send_sem=s_sem, recv_sem=s_sem, device_id=partner, device_id_type=MESH
        ).wait_send()

    def x_piece(k):
        c = pl.ds(k * KC, KC)
        return pltpu.make_async_copy(x_ref.at[:, c], xs.at[h, :, c], x_in.at[k])

    def w_block(i):
        j, k, slot = i // nk, lax.rem(i, nk), lax.rem(i, SLOTS)
        r = pl.ds(pl.multiple_of(k * KC, KC), KC)
        c = pl.ds(pl.multiple_of(h * hw + j * JC, JC), JC)
        return (
            pltpu.make_async_copy(wg_ref.at[r, c], wgb.at[slot], w_in.at[slot, 0]),
            pltpu.make_async_copy(wu_ref.at[r, c], wub.at[slot], w_in.at[slot, 1]),
        )

    def wd_block(c):
        cc = pl.ds(pl.multiple_of(h * cols + c * CW, CW), CW)
        return pltpu.make_async_copy(wd_ref.at[:, cc], wdb.at[c], wd_in.at[c])

    for k in range(nk):
        x_piece(k).start()
    for i in range(SLOTS):
        for cp in w_block(i):
            cp.start()

    barrier = pltpu.get_barrier_semaphore()
    for dev in (partner, *nbr[0], *nbr[1]):
        pl.semaphore_signal(barrier, inc=1, device_id=dev, device_id_type=MESH)
    pl.semaphore_wait(barrier, 5)

    for k in range(nk):
        x_piece(k).wait()
        c = pl.ds(k * KC, KC)
        send(xs.at[h, :, c], xs.at[h, :, c], x_out, x_recv.at[k], partner).start()

    for j in range(nj):
        accg[...] = jnp.zeros_like(accg)
        accu[...] = jnp.zeros_like(accu)

        def block(k, carry, j=j):
            i = j * nk + k
            slot = lax.rem(i, SLOTS)
            kc = pl.ds(pl.multiple_of(k * KC, KC), KC)
            if j == 0:
                landed(xs.at[other, :, kc], x_recv.at[k])
            for cp in w_block(i):
                cp.wait()
            lhs = xs[:, :, kc].reshape(2 * rows, KC)
            accg[...] += jnp.dot(lhs, wgb[slot], preferred_element_type=F32)
            accu[...] += jnp.dot(lhs, wub[slot], preferred_element_type=F32)

            @pl.when(i + SLOTS < nblk)
            def _():
                for cp in w_block(i + SLOTS):
                    cp.start()

            @pl.when((i + SLOTS >= nblk) & (i + SLOTS < nblk + nc))
            def _():
                wd_block(i + SLOTS - nblk).start()

            return carry

        lax.fori_loop(0, nk, block, 0)
        g = accg[...]
        hc = pl.ds(pl.multiple_of(h * hw + j * JC, JC), JC)
        hid[:, hc] = (jax.nn.silu(g) * accu[...]).astype(BF16)
        send(hid.at[:, hc], hid.at[:, hc], h_out, h_recv.at[j], partner).start()
    for c in range(SLOTS, nc):
        wd_block(c).start()
    for j in range(nj):
        hc = pl.ds(pl.multiple_of(other * hw + j * JC, JC), JC)
        landed(hid.at[:, hc], h_recv.at[j])

    def wrap(v):
        return lax.rem(v + 2 * side, side)

    def piece(c, o, b):
        a = coord[o]
        r = pl.ds(pl.multiple_of(a * br + (b // 2) * qr, qr), qr)
        q = pl.ds(pl.multiple_of(c * CW + o * ow + lax.rem(b, 2) * qc, qc), qc)
        return r, q

    def slab(c, o, a):
        r = pl.ds(pl.multiple_of(a * br, br), br)
        q = pl.ds(pl.multiple_of(c * CW + o * ow, ow), ow)
        return r, q

    def scatter_start(src, relay, fin, s_relay, s_fin, q_relay, q_fin, pos, dev):
        send(src.at[wrap(pos + 2), 0], relay.at[0], s_relay, q_relay.at[0], dev[0]).start()
        send(src.at[wrap(pos + 2), 1], relay.at[1], s_relay, q_relay.at[1], dev[1]).start()
        send(src.at[wrap(pos + 1), 1], fin.at[0, 1], s_fin, q_fin.at[0, 1], dev[0]).start()
        send(src.at[wrap(pos - 1), 0], fin.at[1, 0], s_fin, q_fin.at[1, 0], dev[1]).start()

    def scatter_relay(own, relay, fin, s_fin, q_relay, q_fin, pos, dev):
        for d in (0, 1):
            landed(relay.at[d], q_relay.at[d])
            q = wrap(pos + 1 - 2 * d)
            relay[d] = (relay[d].astype(F32) + own[q, d]).astype(BF16)
            send(relay.at[d], fin.at[d, d], s_fin, q_fin.at[d, d], dev[d]).start()

    def scatter_wait(fin, q_fin):
        for d in (0, 1):
            for g in (0, 1):
                landed(fin.at[d, g], q_fin.at[d, g])

    def make_term(c):
        wd_block(c).wait()
        t = jnp.dot(hid[...], wdb[c], preferred_element_type=F32)
        for o in (0, 1):
            for q in range(side):
                for g in (0, 1):
                    v = t[g * rows + q * br:g * rows + (q + 1) * br, o * ow:(o + 1) * ow]
                    term[c, o, q, g] = v
                    termb[c, o, q, g] = v.astype(BF16)
        for o in (0, 1):
            scatter_start(
                termb.at[c, o], r1.at[c, o], f1.at[c, o], s_r1, s_f1, q_r1.at[c, o], q_f1.at[c, o], coord[o], nbr[o]
            )

    def relay_1(c):
        for o in (0, 1):
            scatter_relay(
                term.at[c, o], r1.at[c, o], f1.at[c, o], s_f1, q_r1.at[c, o], q_f1.at[c, o], coord[o], nbr[o]
            )

    def reduce_1(c):
        for o in (0, 1):
            scatter_wait(f1.at[c, o], q_f1.at[c, o])
            for g in (0, 1):
                v = term[c, o, coord[o], g] + f1[c, o, 0, g].astype(F32) + f1[c, o, 1, g].astype(F32)
                for q in range(side):
                    w = v[(q // 2) * qr:(q // 2 + 1) * qr, (q % 2) * qc:(q % 2 + 1) * qc]
                    red[c, o, q, g] = w
                    redb[c, o, q, g] = w.astype(BF16)
            scatter_start(
                redb.at[c, o], r2.at[c, o], f2.at[c, o], s_r2, s_f2, q_r2.at[c, o], q_f2.at[c, o],
                coord[1 - o], nbr[1 - o],
            )

    def relay_2(c):
        for o in (0, 1):
            scatter_relay(
                red.at[c, o], r2.at[c, o], f2.at[c, o], s_f2, q_r2.at[c, o], q_f2.at[c, o], coord[1 - o], nbr[1 - o]
            )

    def reduce_2(c):
        for o in (0, 1):
            scatter_wait(f2.at[c, o], q_f2.at[c, o])
            b = coord[1 - o]

            def total(g):
                v = red[c, o, b, g] + f2[c, o, 0, g].astype(F32) + f2[c, o, 1, g].astype(F32)
                return v.astype(BF16)

            r, q = piece(c, o, b)
            swp[c, o] = total(other)
            send(swp.at[c, o], ybuf.at[h, r, q], s_sw, q_sw.at[c, o], partner).start()
            ybuf[h, r, q] = total(h)

    def gather_1(c):
        for o in (0, 1):
            r, q = piece(c, o, coord[1 - o])
            landed(ybuf.at[other, r, q], q_sw.at[c, o])
            for d in (0, 1):
                send(ybuf.at[:, r, q], ybuf.at[:, r, q], s_g1, q_g1.at[c, o, 0, d], nbr[1 - o][d]).start()

    def forward_1(c):
        for o in (0, 1):
            for d in (0, 1):
                r, q = piece(c, o, wrap(coord[1 - o] - 1 + 2 * d))
                landed(ybuf.at[:, r, q], q_g1.at[c, o, 0, d])
                send(ybuf.at[d, r, q], ybuf.at[d, r, q], s_g1f, q_g1.at[c, o, 1, d], nbr[1 - o][d]).start()

    def gather_2(c):
        for o in (0, 1):
            r, q = piece(c, o, wrap(coord[1 - o] + 2))
            for d in (0, 1):
                landed(ybuf.at[d, r, q], q_g1.at[c, o, 1, d])
            r, q = slab(c, o, coord[o])
            for d in (0, 1):
                send(ybuf.at[:, r, q], ybuf.at[:, r, q], s_g2, q_g2.at[c, o, 0, d], nbr[o][d]).start()

    def forward_2(c):
        for o in (0, 1):
            for d in (0, 1):
                r, q = slab(c, o, wrap(coord[o] - 1 + 2 * d))
                landed(ybuf.at[:, r, q], q_g2.at[c, o, 0, d])
                send(ybuf.at[d, r, q], ybuf.at[d, r, q], s_g2f, q_g2.at[c, o, 1, d], nbr[o][d]).start()

    def finish(c):
        for o in (0, 1):
            r, q = slab(c, o, wrap(coord[o] + 2))
            for d in (0, 1):
                landed(ybuf.at[d, r, q], q_g2.at[c, o, 1, d])
        for d in (0, 1):
            pltpu.make_async_copy(
                ybuf.at[d, :, pl.ds(pl.multiple_of(c * CW, CW), CW)],
                out_ref.at[:, pl.ds(pl.multiple_of(d * cols + c * CW, CW), CW)],
                y_out,
            ).start()

    stages = (
        make_term, relay_1, reduce_1, relay_2, reduce_2, gather_1, forward_1, gather_2, forward_2, finish,
    )

    def tick(t, carry):
        for s, stage in enumerate(stages):
            c = t - s * LAG

            @pl.when((c >= 0) & (c < nc))
            def _(stage=stage, c=c):
                stage(c)

        return carry

    lax.fori_loop(0, nc + (len(stages) - 1) * LAG, tick, 0)

    left_device(ybuf, x_out)
    left_device(hid.at[:, pl.ds(0, hw)], h_out)
    left_device(r1, s_r1)
    left_device(f1, s_f1)
    left_device(r2, s_r2)
    left_device(f2, s_f2)
    left_device(swp, s_sw)
    left_device(f2, s_g1)
    left_device(r2, s_g1f)
    left_device(f1, s_g2)
    left_device(r1, s_g2f)
    pltpu.make_async_copy(ybuf, ybuf, y_out).wait()


def solution(mesh):
    side = math.isqrt(mesh.shape["tp"])

    def step(x, w_gate, w_up, w_down):
        rows, depth = x.shape
        hw = w_gate.shape[1] // 2
        cols = w_down.shape[1] // 2
        nk, nj, nc = depth // KC, hw // JC, cols // CW
        ow = CW // 2
        br, qr, qc = rows // side, rows // side // 2, ow // 2
        dma = pltpu.SemaphoreType.DMA
        scratch = [
            pltpu.VMEM((2, rows, depth), BF16),
            pltpu.VMEM((SLOTS, KC, JC), BF16),
            pltpu.VMEM((SLOTS, KC, JC), BF16),
            pltpu.VMEM((nc, 2 * hw, CW), BF16),
            pltpu.VMEM((2 * rows, JC), F32),
            pltpu.VMEM((2 * rows, JC), F32),
            pltpu.VMEM((2 * rows, 2 * hw), BF16),
            pltpu.VMEM((nc, 2, side, 2, br, ow), F32),
            pltpu.VMEM((nc, 2, side, 2, br, ow), BF16),
            pltpu.VMEM((nc, 2, 2, br, ow), BF16),
            pltpu.VMEM((nc, 2, 2, 2, br, ow), BF16),
            pltpu.VMEM((nc, 2, side, 2, qr, qc), F32),
            pltpu.VMEM((nc, 2, side, 2, qr, qc), BF16),
            pltpu.VMEM((nc, 2, 2, qr, qc), BF16),
            pltpu.VMEM((nc, 2, 2, 2, qr, qc), BF16),
            pltpu.VMEM((nc, 2, qr, qc), BF16),
            pltpu.VMEM((2, rows, cols), BF16),
            dma((nk,)), dma, dma((nk,)), dma((SLOTS, 2)), dma((nc,)), dma, dma((nj,)), dma,
            dma, dma, dma, dma, dma, dma, dma, dma, dma,
            dma((nc, 2, 2)), dma((nc, 2, 2, 2)), dma((nc, 2, 2)), dma((nc, 2, 2, 2)), dma((nc, 2)),
            dma((nc, 2, 2, 2)), dma((nc, 2, 2, 2)),
        ]
        any_spec = pl.BlockSpec(memory_space=pl.ANY)
        return pl.pallas_call(
            functools.partial(kernel, side),
            out_shape=jax.ShapeDtypeStruct((rows, 2 * cols), BF16),
            in_specs=[any_spec] * 4,
            out_specs=any_spec,
            scratch_shapes=scratch,
            compiler_params=pltpu.CompilerParams(
                collective_id=0, has_side_effects=True, vmem_limit_bytes=67_043_328
            ),
            cost_estimate=pl.CostEstimate(
                flops=6 * rows * depth * 2 * hw, bytes_accessed=6 * depth * hw, transcendentals=2 * rows * hw
            ),
        )(x, w_gate, w_up, w_down)

    return jax.shard_map(
        step,
        mesh=mesh,
        in_specs=(P("dp", None), P(None, "tp"), P(None, "tp"), P("tp", None)),
        out_specs=P("dp", None),
        check_vma=False,
    )
```

```python
import functools
import math

import jax
import jax.numpy as jnp
from jax import lax
from jax.experimental import pallas as pl
from jax.experimental.pallas import tpu as pltpu
from jax.sharding import PartitionSpec as P

MESH = pl.DeviceIdType.MESH
F32, BF16 = jnp.float32, jnp.bfloat16

KC = 1024
JC = 512
CW = 512
SLOTS = 8
RING_1 = True
RING_2 = True
LAG = 4


def kernel(
    side, x_ref, wg_ref, wu_ref, wd_ref, out_ref,
    xs, wgb, wub, wdb, accg, accu, hid, term, termb, f1, red, redb, f2, swp, ybuf,
    x_in, x_out, x_recv, w_in, wd_in, h_out, h_recv, y_out,
    s_f1, s_f2, s_sw, s_g1, s_g2, q_f1, q_f2, q_sw, q_g1, q_g2,
):
    rows, depth = x_ref.shape
    hw = wg_ref.shape[1] // 2
    cols = out_ref.shape[1] // 2
    nk, nj, nc = depth // KC, hw // JC, cols // CW
    nblk = nk * nj
    ow = CW // 2
    br, qr, qc = rows // side, rows // side // 2, ow // 2

    dp, tp = lax.axis_index("dp"), lax.axis_index("tp")
    h = lax.rem(dp, 2)
    other = 1 - h
    partner = (dp + 1 - 2 * h, tp)
    cx, cy = tp // side, lax.rem(tp, side)

    def near(axis, d):
        if axis == 0:
            return (dp, lax.rem(cx + d + side, side) * side + cy)
        return (dp, cx * side + lax.rem(cy + d + side, side))

    nbr = [[near(axis, d) for d in (1, -1, 2)] for axis in (0, 1)]
    coord = [cx, cy]

    def send(src, dst, s_sem, r_sem, dev):
        return pltpu.make_async_remote_copy(
            src_ref=src, dst_ref=dst, send_sem=s_sem, recv_sem=r_sem, device_id=dev, device_id_type=MESH
        )

    def landed(dst, r_sem):
        pltpu.make_async_remote_copy(
            src_ref=dst, dst_ref=dst, send_sem=s_sw, recv_sem=r_sem, device_id=partner, device_id_type=MESH
        ).wait_recv()

    def left_device(ref, s_sem):
        pltpu.make_async_remote_copy(
            src_ref=ref, dst_ref=ref, send_sem=s_sem, recv_sem=s_sem, device_id=partner, device_id_type=MESH
        ).wait_send()

    def x_piece(k):
        c = pl.ds(k * KC, KC)
        return pltpu.make_async_copy(x_ref.at[:, c], xs.at[h, :, c], x_in.at[k])

    def w_block(i):
        j, k, slot = i // nk, lax.rem(i, nk), lax.rem(i, SLOTS)
        r = pl.ds(pl.multiple_of(k * KC, KC), KC)
        c = pl.ds(pl.multiple_of(h * hw + j * JC, JC), JC)
        return (
            pltpu.make_async_copy(wg_ref.at[r, c], wgb.at[slot], w_in.at[slot, 0]),
            pltpu.make_async_copy(wu_ref.at[r, c], wub.at[slot], w_in.at[slot, 1]),
        )

    def wd_block(c):
        cc = pl.ds(pl.multiple_of(h * cols + c * CW, CW), CW)
        return pltpu.make_async_copy(wd_ref.at[:, cc], wdb.at[c], wd_in.at[c])

    for k in range(nk):
        x_piece(k).start()
    for i in range(SLOTS):
        for cp in w_block(i):
            cp.start()

    barrier = pltpu.get_barrier_semaphore()
    for dev in (partner, *nbr[0], *nbr[1]):
        pl.semaphore_signal(barrier, inc=1, device_id=dev, device_id_type=MESH)
    pl.semaphore_wait(barrier, 7)

    for k in range(nk):
        x_piece(k).wait()
        c = pl.ds(k * KC, KC)
        send(xs.at[h, :, c], xs.at[h, :, c], x_out, x_recv.at[k], partner).start()

    for j in range(nj):
        accg[...] = jnp.zeros_like(accg)
        accu[...] = jnp.zeros_like(accu)

        def block(k, carry, j=j):
            i = j * nk + k
            slot = lax.rem(i, SLOTS)
            kc = pl.ds(pl.multiple_of(k * KC, KC), KC)
            if j == 0:
                landed(xs.at[other, :, kc], x_recv.at[k])
            for cp in w_block(i):
                cp.wait()
            lhs = xs[:, :, kc].reshape(2 * rows, KC)
            accg[...] += jnp.dot(lhs, wgb[slot], preferred_element_type=F32)
            accu[...] += jnp.dot(lhs, wub[slot], preferred_element_type=F32)

            @pl.when(i + SLOTS < nblk)
            def _():
                for cp in w_block(i + SLOTS):
                    cp.start()

            @pl.when((i + SLOTS >= nblk) & (i + SLOTS < nblk + nc))
            def _():
                wd_block(i + SLOTS - nblk).start()

            return carry

        lax.fori_loop(0, nk, block, 0)
        g = accg[...]
        hc = pl.ds(pl.multiple_of(h * hw + j * JC, JC), JC)
        hid[:, hc] = (jax.nn.silu(g) * accu[...]).astype(BF16)
        send(hid.at[:, hc], hid.at[:, hc], h_out, h_recv.at[j], partner).start()
    for c in range(SLOTS, nc):
        wd_block(c).start()
    for j in range(nj):
        hc = pl.ds(pl.multiple_of(other * hw + j * JC, JC), JC)
        landed(hid.at[:, hc], h_recv.at[j])

    def wrap(v):
        return lax.rem(v + 2 * side, side)

    def piece(c, o, b):
        a = coord[o]
        r = pl.ds(pl.multiple_of(a * br + (b // 2) * qr, qr), qr)
        q = pl.ds(pl.multiple_of(c * CW + o * ow + lax.rem(b, 2) * qc, qc), qc)
        return r, q

    def slab(c, o, a):
        r = pl.ds(pl.multiple_of(a * br, br), br)
        q = pl.ds(pl.multiple_of(c * CW + o * ow, ow), ow)
        return r, q

    def scatter_direct(src, fin, s_fin, sem, pos, dev):
        for d, delta in enumerate((1, -1, 2)):
            send(src.at[wrap(pos + delta)], fin.at[d], s_fin, sem(d), dev[d]).start()

    def scatter_ring(src, fin, s_fin, q_fin, pos, dev):
        for d in (0, 1):
            send(src.at[wrap(pos + 2), d], fin.at[2, d], s_fin, q_fin.at[2, d], dev[d]).start()
        for d in (0, 1):
            send(src.at[wrap(pos + 1 - 2 * d), 1 - d], fin.at[d, 1 - d], s_fin, q_fin.at[d, 1 - d], dev[d]).start()

    def make_term(c):
        wd_block(c).wait()
        t = jnp.dot(hid[...], wdb[c], preferred_element_type=F32)
        for o in (0, 1):
            for q in range(side):
                for g in (0, 1):
                    v = t[g * rows + q * br:g * rows + (q + 1) * br, o * ow:(o + 1) * ow]
                    term[c, o, q, g] = v
                    termb[c, o, q, g] = v.astype(BF16)
        for o in (0, 1):
            if RING_1:
                scatter_ring(termb.at[c, o], f1.at[c, o], s_f1, q_f1.at[c, o], coord[o], nbr[o])
            else:
                scatter_direct(
                    termb.at[c, o], f1.at[c, o], s_f1, lambda d, o=o: q_f1.at[c, o, d, 0], coord[o], nbr[o]
                )

    def relay_1(c):
        for o in (0, 1):
            for d in (0, 1):
                part = f1.at[c, o, 2, d]
                landed(part, q_f1.at[c, o, 2, d])
                part[...] = (part[...].astype(F32) + term[c, o, wrap(coord[o] + 1 - 2 * d), d]).astype(BF16)
                send(part, f1.at[c, o, d, d], s_f1, q_f1.at[c, o, d, d], nbr[o][d]).start()

    def reduce_1(c):
        for o in (0, 1):
            if RING_1:
                for d in (0, 1):
                    for g in (0, 1):
                        landed(f1.at[c, o, d, g], q_f1.at[c, o, d, g])
            else:
                for d in range(3):
                    landed(f1.at[c, o, d], q_f1.at[c, o, d, 0])
            for g in (0, 1):
                v = term[c, o, coord[o], g] + f1[c, o, 0, g].astype(F32) + f1[c, o, 1, g].astype(F32)
                if not RING_1:
                    v = v + f1[c, o, 2, g].astype(F32)
                for q in range(side):
                    w = v[(q // 2) * qr:(q // 2 + 1) * qr, (q % 2) * qc:(q % 2 + 1) * qc]
                    red[c, o, q, g] = w
                    redb[c, o, q, g] = w.astype(BF16)
            scatter_direct(
                redb.at[c, o], f2.at[c, o], s_f2, lambda d, o=o: q_f2.at[c, o, d], coord[1 - o], nbr[1 - o]
            )

    def reduce_2(c):
        for o in (0, 1):
            b = coord[1 - o]
            for d in range(3):
                landed(f2.at[c, o, d], q_f2.at[c, o, d])

            def total(g):
                v = red[c, o, b, g] + f2[c, o, 0, g].astype(F32) + f2[c, o, 1, g].astype(F32)
                return (v + f2[c, o, 2, g].astype(F32)).astype(BF16)

            r, q = piece(c, o, b)
            swp[c, o] = total(other)
            send(swp.at[c, o], ybuf.at[h, r, q], s_sw, q_sw.at[c, o], partner).start()
            ybuf[h, r, q] = total(h)

    def gather_1(c):
        for o in (0, 1):
            r, q = piece(c, o, coord[1 - o])
            landed(ybuf.at[other, r, q], q_sw.at[c, o])
            for d in range(3):
                send(ybuf.at[:, r, q], ybuf.at[:, r, q], s_g1, q_g1.at[c, o, d], nbr[1 - o][d]).start()

    def gather_2(c):
        for o in (0, 1):
            for d, delta in enumerate((-1, 1, 2)):
                r, q = piece(c, o, wrap(coord[1 - o] + delta))
                landed(ybuf.at[:, r, q], q_g1.at[c, o, d])
            r, q = slab(c, o, coord[o])
            for d in range(2 if RING_2 else 3):
                send(ybuf.at[:, r, q], ybuf.at[:, r, q], s_g2, q_g2.at[c, o, d % 2, d // 2], nbr[o][d]).start()

    def forward_2(c):
        for o in (0, 1):
            for d in (0, 1):
                r, q = slab(c, o, wrap(coord[o] - 1 + 2 * d))
                landed(ybuf.at[:, r, q], q_g2.at[c, o, d, 0])
                send(ybuf.at[d, r, q], ybuf.at[d, r, q], s_g2, q_g2.at[c, o, d, 1], nbr[o][d]).start()

    def finish(c):
        for o in (0, 1):
            if RING_2:
                r, q = slab(c, o, wrap(coord[o] + 2))
                for d in (0, 1):
                    landed(ybuf.at[d, r, q], q_g2.at[c, o, d, 1])
            else:
                for d, delta in enumerate((-1, 1, 2)):
                    r, q = slab(c, o, wrap(coord[o] + delta))
                    landed(ybuf.at[:, r, q], q_g2.at[c, o, d % 2, d // 2])
        for d in (0, 1):
            pltpu.make_async_copy(
                ybuf.at[d, :, pl.ds(pl.multiple_of(c * CW, CW), CW)],
                out_ref.at[:, pl.ds(pl.multiple_of(d * cols + c * CW, CW), CW)],
                y_out,
            ).start()

    stages = [make_term] + [relay_1] * RING_1 + [reduce_1, reduce_2, gather_1, gather_2] + [forward_2] * RING_2 + [finish]

    def tick(t, carry):
        for s, stage in enumerate(stages):
            c = t - s * LAG

            @pl.when((c >= 0) & (c < nc))
            def _(stage=stage, c=c):
                stage(c)

        return carry

    lax.fori_loop(0, nc + (len(stages) - 1) * LAG, tick, 0)

    left_device(ybuf, x_out)
    left_device(hid.at[:, pl.ds(0, hw)], h_out)
    left_device(f1, s_f1)
    left_device(f2, s_f2)
    left_device(swp, s_sw)
    left_device(f2, s_g1)
    left_device(f1, s_g2)
    pltpu.make_async_copy(ybuf, ybuf, y_out).wait()


def solution(mesh):
    side = math.isqrt(mesh.shape["tp"])

    def step(x, w_gate, w_up, w_down):
        rows, depth = x.shape
        hw = w_gate.shape[1] // 2
        cols = w_down.shape[1] // 2
        nk, nj, nc = depth // KC, hw // JC, cols // CW
        ow = CW // 2
        br, qr, qc = rows // side, rows // side // 2, ow // 2
        dma = pltpu.SemaphoreType.DMA
        scratch = [
            pltpu.VMEM((2, rows, depth), BF16),
            pltpu.VMEM((SLOTS, KC, JC), BF16),
            pltpu.VMEM((SLOTS, KC, JC), BF16),
            pltpu.VMEM((nc, 2 * hw, CW), BF16),
            pltpu.VMEM((2 * rows, JC), F32),
            pltpu.VMEM((2 * rows, JC), F32),
            pltpu.VMEM((2 * rows, 2 * hw), BF16),
            pltpu.VMEM((nc, 2, side, 2, br, ow), F32),
            pltpu.VMEM((nc, 2, side, 2, br, ow), BF16),
            pltpu.VMEM((nc, 2, 3, 2, br, ow), BF16),
            pltpu.VMEM((nc, 2, side, 2, qr, qc), F32),
            pltpu.VMEM((nc, 2, side, 2, qr, qc), BF16),
            pltpu.VMEM((nc, 2, 3, 2, qr, qc), BF16),
            pltpu.VMEM((nc, 2, qr, qc), BF16),
            pltpu.VMEM((2, rows, cols), BF16),
            dma((nk,)), dma, dma((nk,)), dma((SLOTS, 2)), dma((nc,)), dma, dma((nj,)), dma,
            dma, dma, dma, dma, dma,
            dma((nc, 2, 3, 2)), dma((nc, 2, 3)), dma((nc, 2)), dma((nc, 2, 3)), dma((nc, 2, 2, 2)),
        ]
        any_spec = pl.BlockSpec(memory_space=pl.ANY)
        return pl.pallas_call(
            functools.partial(kernel, side),
            out_shape=jax.ShapeDtypeStruct((rows, 2 * cols), BF16),
            in_specs=[any_spec] * 4,
            out_specs=any_spec,
            scratch_shapes=scratch,
            compiler_params=pltpu.CompilerParams(
                collective_id=0, has_side_effects=True, vmem_limit_bytes=67_043_328
            ),
            cost_estimate=pl.CostEstimate(
                flops=6 * rows * depth * 2 * hw, bytes_accessed=6 * depth * hw, transcendentals=2 * rows * hw
            ),
        )(x, w_gate, w_up, w_down)

    return jax.shard_map(
        step,
        mesh=mesh,
        in_specs=(P("dp", None), P(None, "tp"), P(None, "tp"), P("tp", None)),
        out_specs=P("dp", None),
        check_vma=False,
    )
```

```python
import functools
import math

import jax
import jax.numpy as jnp
from jax import lax
from jax.experimental import pallas as pl
from jax.experimental.pallas import tpu as pltpu
from jax.sharding import PartitionSpec as P

MESH = pl.DeviceIdType.MESH
F32, BF16 = jnp.float32, jnp.bfloat16

VMEM_LIMIT = 51 << 20
KC = 1024
JC = 512
CW = 512
FIRST = 2
DEPTH = 6
AHEAD = 4
RING_1 = True
RING_2 = True
LAG = 4


def kernel(
    side, x_ref, wg_ref, wu_ref, wd_ref, ybuf,
    xs, pool, acc, hid, term, termb, f1, red, redb, f2, swp,
    x_in, x_out, x_recv, w_in, wd_in, h_out, h_recv,
    s_f1, s_f2, s_sw, s_g1, s_g2, q_f1, q_f2, q_sw, q_g1, q_g2,
):
    rows, depth = x_ref.shape
    hw = wg_ref.shape[1] // 2
    cols = ybuf.shape[2]
    nk, nj, nc = depth // KC, hw // JC, cols // CW
    nblk = nk * nj
    ow = CW // 2
    br, qr, qc = rows // side, rows // side // 2, ow // 2

    dp, tp = lax.axis_index("dp"), lax.axis_index("tp")
    h = lax.rem(dp, 2)
    other = 1 - h
    partner = (dp + 1 - 2 * h, tp)
    cx, cy = tp // side, lax.rem(tp, side)

    def near(axis, d):
        if axis == 0:
            return (dp, lax.rem(cx + d + side, side) * side + cy)
        return (dp, cx * side + lax.rem(cy + d + side, side))

    nbr = [[near(axis, d) for d in (1, -1, 2)] for axis in (0, 1)]
    coord = [cx, cy]

    def send(src, dst, s_sem, r_sem, dev):
        return pltpu.make_async_remote_copy(
            src_ref=src, dst_ref=dst, send_sem=s_sem, recv_sem=r_sem, device_id=dev, device_id_type=MESH
        )

    def landed(dst, r_sem):
        pltpu.make_async_remote_copy(
            src_ref=dst, dst_ref=dst, send_sem=s_sw, recv_sem=r_sem, device_id=partner, device_id_type=MESH
        ).wait_recv()

    def left_device(ref, s_sem):
        pltpu.make_async_remote_copy(
            src_ref=ref, dst_ref=ref, send_sem=s_sem, recv_sem=s_sem, device_id=partner, device_id_type=MESH
        ).wait_send()

    def x_piece(k):
        c = pl.ds(k * KC, KC)
        return pltpu.make_async_copy(x_ref.at[:, c], xs.at[h, :, c], x_in.at[k])

    def w_block(i):
        j, k = i // nk, lax.rem(i, nk)
        r = pl.ds(pl.multiple_of(k * KC, KC), KC)
        c = pl.ds(pl.multiple_of(h * hw + j * JC, JC), JC)
        return [
            pltpu.make_async_copy(ref.at[r, c], pool.at[i, m], w_in.at[i, m]) for m, ref in enumerate((wg_ref, wu_ref))
        ]

    def wd_block(c):
        cc = pl.ds(pl.multiple_of(h * cols + c * CW, CW), CW)
        return [
            pltpu.make_async_copy(wd_ref.at[pl.ds(m * hw, hw), cc], pool.at[c, m], wd_in.at[c, m]) for m in (0, 1)
        ]

    def wait_all(copies):
        for cp in copies:
            cp.wait()

    def start_all(copies):
        for cp in copies:
            cp.start()

    barrier = pltpu.get_barrier_semaphore()
    for dev in (partner, *nbr[0], *nbr[1]):
        pl.semaphore_signal(barrier, inc=1, device_id=dev, device_id_type=MESH)

    for k in range(nk):
        x_piece(k).start()
    for i in range(FIRST):
        start_all(w_block(i))
    acc[...] = jnp.zeros_like(acc)

    def chunk_of_x(k):
        return pl.ds(pl.multiple_of(k * KC, KC), KC)

    def following(i):
        @pl.when(i < nblk)
        def _():
            start_all(w_block(i))

        @pl.when(i >= nblk)
        def _():
            start_all(wd_block(i - nblk))

    def all_rows(j, k):
        wait_all(w_block(j * nk + k))
        following(j * nk + k + DEPTH)
        lhs = xs[:, :, chunk_of_x(k)].reshape(2 * rows, KC)
        for m in (0, 1):
            acc[j, m] += jnp.dot(lhs, pool[j * nk + k, m], preferred_element_type=F32).reshape(2, rows, JC)

    def send_hidden(j, n, width):
        c = pl.ds(pl.multiple_of(h * hw + j * JC + n * width, width), width)
        send(hid.at[:, c], hid.at[:, c], h_out, h_recv.at[j + n], partner).start()

    pl.semaphore_wait(barrier, 7)
    for k in range(nk):
        x_piece(k).wait()
        c = pl.ds(k * KC, KC)
        send(xs.at[h, :, c], xs.at[h, :, c], x_out, x_recv.at[k], partner).start()
    for i in range(FIRST, DEPTH):
        start_all(w_block(i))

    def first_half(k, carry):
        landed(xs.at[other, :, chunk_of_x(k)], x_recv.at[k])
        all_rows(0, k)
        return carry

    lax.fori_loop(0, nk, first_half, 0)

    def with_act(t, carry):
        all_rows(1, t)
        hc = pl.ds(pl.multiple_of(h * hw, JC), JC)
        hid[pl.ds(pl.multiple_of(t * rows, rows), rows), hc] = (
            jax.nn.silu(acc[0, 0, t]) * acc[0, 1, t]
        ).astype(BF16)
        return carry

    lax.fori_loop(0, 2, with_act, 0)
    send_hidden(0, 0, JC)

    def second_half(k, carry):
        all_rows(1, k)
        return carry

    lax.fori_loop(2, nk - 1, second_half, 0)
    k = nk - 1
    wait_all(w_block(nk + k))
    following(nk + k + DEPTH)
    lhs = xs[:, :, chunk_of_x(k)].reshape(2 * rows, KC)
    half = JC // 2
    for n in (0, 1):
        cc = slice(n * half, (n + 1) * half)
        g, u = (
            acc[1, m, :, :, cc].reshape(2 * rows, half)
            + jnp.dot(lhs, pool[nk + k, m, :, cc], preferred_element_type=F32)
            for m in (0, 1)
        )
        hid[:, pl.ds(pl.multiple_of(h * hw + JC + n * half, half), half)] = (jax.nn.silu(g) * u).astype(BF16)
        send_hidden(1, n, half)

    mine = pl.ds(pl.multiple_of(h * hw, hw), hw)
    theirs = pl.ds(pl.multiple_of(other * hw, hw), hw)

    def own_half(c):
        wait_all(wd_block(c))

        @pl.when(c + DEPTH < nc)
        def _():
            start_all(wd_block(c + DEPTH))

        t = jnp.dot(hid[:, mine], pool[c, h], preferred_element_type=F32)
        for o in (0, 1):
            for q in range(side):
                for g in (0, 1):
                    term[c, o, q, g] = t[g * rows + q * br:g * rows + (q + 1) * br, o * ow:(o + 1) * ow]

    def ahead(c, carry):
        own_half(c)
        return carry

    lax.fori_loop(0, AHEAD, ahead, 0)
    for j, n, width in ((0, 0, JC), (1, 0, half), (1, 1, half)):
        c = pl.ds(pl.multiple_of(other * hw + j * JC + n * width, width), width)
        landed(hid.at[:, c], h_recv.at[j + n])

    def wrap(v):
        return lax.rem(v + 2 * side, side)

    def piece(c, o, b):
        a = coord[o]
        r = pl.ds(pl.multiple_of(a * br + (b // 2) * qr, qr), qr)
        q = pl.ds(pl.multiple_of(c * CW + o * ow + lax.rem(b, 2) * qc, qc), qc)
        return r, q

    def slab(c, o, a):
        r = pl.ds(pl.multiple_of(a * br, br), br)
        q = pl.ds(pl.multiple_of(c * CW + o * ow, ow), ow)
        return r, q

    def scatter_direct(src, fin, s_fin, sem, pos, dev):
        for d, delta in enumerate((1, -1, 2)):
            send(src.at[wrap(pos + delta)], fin.at[d], s_fin, sem(d), dev[d]).start()

    def scatter_ring(src, fin, s_fin, q_fin, pos, dev):
        for d in (0, 1):
            send(src.at[wrap(pos + 2), d], fin.at[2, d], s_fin, q_fin.at[2, d], dev[d]).start()
        for d in (0, 1):
            send(src.at[wrap(pos + 1 - 2 * d), 1 - d], fin.at[d, 1 - d], s_fin, q_fin.at[d, 1 - d], dev[d]).start()

    def make_term(c):
        t = jnp.dot(hid[:, theirs], pool[c, other], preferred_element_type=F32)
        for o in (0, 1):
            for q in range(side):
                for g in (0, 1):
                    v = t[g * rows + q * br:g * rows + (q + 1) * br, o * ow:(o + 1) * ow]
                    v = v + term[c, o, q, g]
                    term[c, o, q, g] = v
                    termb[c, o, q, g] = v.astype(BF16)
        for o in (0, 1):
            if RING_1:
                scatter_ring(termb.at[c, o], f1.at[c, o], s_f1, q_f1.at[c, o], coord[o], nbr[o])
            else:
                scatter_direct(
                    termb.at[c, o], f1.at[c, o], s_f1, lambda d, o=o: q_f1.at[c, o, d, 0], coord[o], nbr[o]
                )

        @pl.when(c + AHEAD < nc)
        def _():
            own_half(c + AHEAD)

    def relay_1(c):
        for o in (0, 1):
            for d in (0, 1):
                part = f1.at[c, o, 2, d]
                landed(part, q_f1.at[c, o, 2, d])
                part[...] = (part[...].astype(F32) + term[c, o, wrap(coord[o] + 1 - 2 * d), d]).astype(BF16)
                send(part, f1.at[c, o, d, d], s_f1, q_f1.at[c, o, d, d], nbr[o][d]).start()

    def reduce_1(c):
        for o in (0, 1):
            if RING_1:
                for d in (0, 1):
                    for g in (0, 1):
                        landed(f1.at[c, o, d, g], q_f1.at[c, o, d, g])
            else:
                for d in range(3):
                    landed(f1.at[c, o, d], q_f1.at[c, o, d, 0])
            for g in (0, 1):
                v = term[c, o, coord[o], g] + f1[c, o, 0, g].astype(F32) + f1[c, o, 1, g].astype(F32)
                if not RING_1:
                    v = v + f1[c, o, 2, g].astype(F32)
                for q in range(side):
                    w = v[(q // 2) * qr:(q // 2 + 1) * qr, (q % 2) * qc:(q % 2 + 1) * qc]
                    red[c, o, q, g] = w
                    redb[c, o, q, g] = w.astype(BF16)
            scatter_direct(
                redb.at[c, o], f2.at[c, o], s_f2, lambda d, o=o: q_f2.at[c, o, d], coord[1 - o], nbr[1 - o]
            )

    def reduce_2(c):
        for o in (0, 1):
            b = coord[1 - o]
            for d in range(3):
                landed(f2.at[c, o, d], q_f2.at[c, o, d])

            def total(g):
                v = red[c, o, b, g] + f2[c, o, 0, g].astype(F32) + f2[c, o, 1, g].astype(F32)
                return (v + f2[c, o, 2, g].astype(F32)).astype(BF16)

            r, q = piece(c, o, b)
            swp[c, o] = total(other)
            send(swp.at[c, o], ybuf.at[h, r, q], s_sw, q_sw.at[c, o], partner).start()
            ybuf[h, r, q] = total(h)

    def gather_1(c):
        for o in (0, 1):
            r, q = piece(c, o, coord[1 - o])
            landed(ybuf.at[other, r, q], q_sw.at[c, o])
            for d in range(3):
                send(ybuf.at[:, r, q], ybuf.at[:, r, q], s_g1, q_g1.at[c, o, d], nbr[1 - o][d]).start()

    def gather_2(c):
        for o in (0, 1):
            for d, delta in enumerate((-1, 1, 2)):
                r, q = piece(c, o, wrap(coord[1 - o] + delta))
                landed(ybuf.at[:, r, q], q_g1.at[c, o, d])
            r, q = slab(c, o, coord[o])
            for d in range(2 if RING_2 else 3):
                send(ybuf.at[:, r, q], ybuf.at[:, r, q], s_g2, q_g2.at[c, o, d % 2, d // 2], nbr[o][d]).start()

    def forward_2(c):
        for o in (0, 1):
            for d in (0, 1):
                r, q = slab(c, o, wrap(coord[o] - 1 + 2 * d))
                landed(ybuf.at[:, r, q], q_g2.at[c, o, d, 0])
                send(ybuf.at[d, r, q], ybuf.at[d, r, q], s_g2, q_g2.at[c, o, d, 1], nbr[o][d]).start()

    def finish(c):
        for o in (0, 1):
            if RING_2:
                r, q = slab(c, o, wrap(coord[o] + 2))
                for d in (0, 1):
                    landed(ybuf.at[d, r, q], q_g2.at[c, o, d, 1])
            else:
                for d, delta in enumerate((-1, 1, 2)):
                    r, q = slab(c, o, wrap(coord[o] + delta))
                    landed(ybuf.at[:, r, q], q_g2.at[c, o, d % 2, d // 2])

    stages = [make_term] + [relay_1] * RING_1 + [reduce_1, reduce_2, gather_1, gather_2] + [forward_2] * RING_2 + [finish]

    def tick(t, carry):
        for s, stage in enumerate(stages):
            c = t - s * LAG

            @pl.when((c >= 0) & (c < nc))
            def _(stage=stage, c=c):
                stage(c)

        return carry

    lax.fori_loop(0, nc + (len(stages) - 1) * LAG, tick, 0)

    left_device(ybuf, x_out)
    left_device(hid.at[:, pl.ds(0, hw)], h_out)
    left_device(f1, s_f1)
    left_device(f2, s_f2)
    left_device(swp, s_sw)
    left_device(f2, s_g1)
    left_device(f1, s_g2)


def write_out(y_ref, out_ref, sem):
    rows, cols = y_ref.shape[1:]
    n = sem.shape[1]
    copies = [
        pltpu.make_async_copy(
            y_ref.at[d, pl.ds(i * rows // n, rows // n)],
            out_ref.at[pl.ds(i * rows // n, rows // n), pl.ds(d * cols, cols)],
            sem.at[d, i],
        )
        for d in (0, 1)
        for i in range(n)
    ]
    for cp in copies:
        cp.start()
    for cp in copies:
        cp.wait()


def solution(mesh):
    side = math.isqrt(mesh.shape["tp"])

    def step(x, w_gate, w_up, w_down):
        rows, depth = x.shape
        hw = w_gate.shape[1] // 2
        cols = w_down.shape[1] // 2
        nk, nj, nc = depth // KC, hw // JC, cols // CW
        ow = CW // 2
        br, qr, qc = rows // side, rows // side // 2, ow // 2
        dma = pltpu.SemaphoreType.DMA
        scratch = [
            pltpu.VMEM((2, rows, depth), BF16),
            pltpu.VMEM((nk * nj, 2, KC, JC), BF16),
            pltpu.VMEM((nj, 2, 2, rows, JC), F32),
            pltpu.VMEM((2 * rows, 2 * hw), BF16),
            pltpu.VMEM((nc, 2, side, 2, br, ow), F32),
            pltpu.VMEM((nc, 2, side, 2, br, ow), BF16),
            pltpu.VMEM((nc, 2, 3, 2, br, ow), BF16),
            pltpu.VMEM((nc, 2, side, 2, qr, qc), F32),
            pltpu.VMEM((nc, 2, side, 2, qr, qc), BF16),
            pltpu.VMEM((nc, 2, 3, 2, qr, qc), BF16),
            pltpu.VMEM((nc, 2, qr, qc), BF16),
            dma((nk,)), dma, dma((nk,)), dma((nk * nj, 2)), dma((nc, 2)), dma, dma((nj + 1,)),
            dma, dma, dma, dma, dma,
            dma((nc, 2, 3, 2)), dma((nc, 2, 3)), dma((nc, 2)), dma((nc, 2, 3)), dma((nc, 2, 2, 2)),
        ]
        any_spec = pl.BlockSpec(memory_space=pl.ANY)
        y = pl.pallas_call(
            functools.partial(kernel, side),
            out_shape=jax.ShapeDtypeStruct((2, rows, cols), BF16),
            in_specs=[any_spec] * 4,
            out_specs=pl.BlockSpec(memory_space=pltpu.VMEM),
            scratch_shapes=scratch,
            compiler_params=pltpu.CompilerParams(
                collective_id=0, has_side_effects=True, vmem_limit_bytes=VMEM_LIMIT
            ),
            cost_estimate=pl.CostEstimate(
                flops=6 * rows * depth * 2 * hw, bytes_accessed=6 * depth * hw, transcendentals=2 * rows * hw
            ),
        )(pltpu.with_memory_space_constraint(x, pltpu.HBM), w_gate, w_up, w_down)
        return pl.pallas_call(
            write_out,
            out_shape=jax.ShapeDtypeStruct((rows, 2 * cols), BF16),
            in_specs=[pl.BlockSpec(memory_space=pltpu.VMEM)],
            out_specs=any_spec,
            scratch_shapes=[dma((2, 4))],
            compiler_params=pltpu.CompilerParams(vmem_limit_bytes=1 << 20),
        )(y)

    return jax.shard_map(
        step,
        mesh=mesh,
        in_specs=(P("dp", None), P(None, "tp"), P(None, "tp"), P("tp", None)),
        out_specs=P("dp", None),
        check_vma=False,
    )
```

```python
import functools
import math

import jax
import jax.numpy as jnp
from jax import lax
from jax.experimental import pallas as pl
from jax.experimental.pallas import tpu as pltpu
from jax.sharding import PartitionSpec as P

MESH = pl.DeviceIdType.MESH
F32, BF16 = jnp.float32, jnp.bfloat16

VMEM_LIMIT = 51 << 20
KC = 1024
JC = 512
CW = 512
FIRST = 2
DEPTH = 6
AHEAD = 2
STRAIGHT_1 = 0
STRAIGHT_2 = 2
LAG = 6


def kernel(
    side, x_ref, wg_ref, wu_ref, wd_ref, ybuf,
    xs, pool, acc, hid, term, termb, f1, red, redb, f2, swp,
    x_in, x_out, x_recv, w_in, wd_in, h_out, h_recv,
    s_f1, s_f2, s_sw, s_g1, s_g2, q_f1, q_f2, q_sw, q_g1, q_g2,
):
    rows, depth = x_ref.shape
    hw = wg_ref.shape[1] // 2
    cols = ybuf.shape[2]
    nk, nj, nc = depth // KC, hw // JC, cols // CW
    nblk = nk * nj
    ow = CW // 2
    br, qr, qc = rows // side, rows // side // 2, ow // 2

    dp, tp = lax.axis_index("dp"), lax.axis_index("tp")
    h = lax.rem(dp, 2)
    other = 1 - h
    partner = (dp + 1 - 2 * h, tp)
    cx, cy = tp // side, lax.rem(tp, side)

    def near(axis, d):
        if axis == 0:
            return (dp, lax.rem(cx + d + side, side) * side + cy)
        return (dp, cx * side + lax.rem(cy + d + side, side))

    nbr = [[near(axis, d) for d in (1, -1, 2)] for axis in (0, 1)]
    coord = [cx, cy]

    def send(src, dst, s_sem, r_sem, dev):
        return pltpu.make_async_remote_copy(
            src_ref=src, dst_ref=dst, send_sem=s_sem, recv_sem=r_sem, device_id=dev, device_id_type=MESH
        )

    def landed(dst, r_sem):
        pltpu.make_async_remote_copy(
            src_ref=dst, dst_ref=dst, send_sem=s_sw, recv_sem=r_sem, device_id=partner, device_id_type=MESH
        ).wait_recv()

    def left_device(ref, s_sem):
        pltpu.make_async_remote_copy(
            src_ref=ref, dst_ref=ref, send_sem=s_sem, recv_sem=s_sem, device_id=partner, device_id_type=MESH
        ).wait_send()

    def x_piece(k):
        c = pl.ds(k * KC, KC)
        return pltpu.make_async_copy(x_ref.at[:, c], xs.at[h, :, c], x_in.at[k])

    def w_block(i):
        j, k = i // nk, lax.rem(i, nk)
        r = pl.ds(pl.multiple_of(k * KC, KC), KC)
        c = pl.ds(pl.multiple_of(h * hw + j * JC, JC), JC)
        return [
            pltpu.make_async_copy(ref.at[r, c], pool.at[i, m], w_in.at[i, m]) for m, ref in enumerate((wg_ref, wu_ref))
        ]

    def wd_block(c):
        cc = pl.ds(pl.multiple_of(h * cols + c * CW, CW), CW)
        return [
            pltpu.make_async_copy(wd_ref.at[pl.ds(m * hw, hw), cc], pool.at[c, m], wd_in.at[c, m]) for m in (0, 1)
        ]

    def wait_all(copies):
        for cp in copies:
            cp.wait()

    def start_all(copies):
        for cp in copies:
            cp.start()

    barrier = pltpu.get_barrier_semaphore()
    for dev in (partner, *nbr[0], *nbr[1]):
        pl.semaphore_signal(barrier, inc=1, device_id=dev, device_id_type=MESH)

    for k in range(nk):
        x_piece(k).start()
    for i in range(FIRST):
        start_all(w_block(i))
    acc[...] = jnp.zeros_like(acc)

    def chunk_of_x(k):
        return pl.ds(pl.multiple_of(k * KC, KC), KC)

    def following(i):
        @pl.when(i < nblk)
        def _():
            start_all(w_block(i))

        @pl.when(i >= nblk)
        def _():
            start_all(wd_block(i - nblk))

    def all_rows(j, k):
        wait_all(w_block(j * nk + k))
        following(j * nk + k + DEPTH)
        lhs = xs[:, :, chunk_of_x(k)].reshape(2 * rows, KC)
        for m in (0, 1):
            acc[j, m] += jnp.dot(lhs, pool[j * nk + k, m], preferred_element_type=F32).reshape(2, rows, JC)

    def send_hidden(j, n, width):
        c = pl.ds(pl.multiple_of(h * hw + j * JC + n * width, width), width)
        send(hid.at[:, c], hid.at[:, c], h_out, h_recv.at[j + n], partner).start()

    pl.semaphore_wait(barrier, 7)
    for k in range(nk):
        x_piece(k).wait()
        c = pl.ds(k * KC, KC)
        send(xs.at[h, :, c], xs.at[h, :, c], x_out, x_recv.at[k], partner).start()
    for i in range(FIRST, DEPTH):
        start_all(w_block(i))

    def first_half(k, carry):
        landed(xs.at[other, :, chunk_of_x(k)], x_recv.at[k])
        all_rows(0, k)
        return carry

    lax.fori_loop(0, nk, first_half, 0)

    def with_act(t, carry):
        all_rows(1, t)
        hc = pl.ds(pl.multiple_of(h * hw, JC), JC)
        hid[pl.ds(pl.multiple_of(t * rows, rows), rows), hc] = (
            jax.nn.silu(acc[0, 0, t]) * acc[0, 1, t]
        ).astype(BF16)
        return carry

    lax.fori_loop(0, 2, with_act, 0)
    send_hidden(0, 0, JC)

    def second_half(k, carry):
        all_rows(1, k)
        return carry

    lax.fori_loop(2, nk - 1, second_half, 0)
    k = nk - 1
    wait_all(w_block(nk + k))
    following(nk + k + DEPTH)
    lhs = xs[:, :, chunk_of_x(k)].reshape(2 * rows, KC)
    half = JC // 2
    for n in (0, 1):
        cc = slice(n * half, (n + 1) * half)
        g, u = (
            acc[1, m, :, :, cc].reshape(2 * rows, half)
            + jnp.dot(lhs, pool[nk + k, m, :, cc], preferred_element_type=F32)
            for m in (0, 1)
        )
        hid[:, pl.ds(pl.multiple_of(h * hw + JC + n * half, half), half)] = (jax.nn.silu(g) * u).astype(BF16)
        send_hidden(1, n, half)

    mine = pl.ds(pl.multiple_of(h * hw, hw), hw)
    theirs = pl.ds(pl.multiple_of(other * hw, hw), hw)

    def own_half(c):
        wait_all(wd_block(c))

        @pl.when(c + DEPTH < nc)
        def _():
            start_all(wd_block(c + DEPTH))

        t = jnp.dot(hid[:, mine], pool[c, h], preferred_element_type=F32)
        for o in (0, 1):
            for q in range(side):
                for g in (0, 1):
                    term[c, o, q, g] = t[g * rows + q * br:g * rows + (q + 1) * br, o * ow:(o + 1) * ow]

    def ahead(c, carry):
        own_half(c)
        return carry

    lax.fori_loop(0, AHEAD, ahead, 0)
    for j, n, width in ((0, 0, JC), (1, 0, half), (1, 1, half)):
        c = pl.ds(pl.multiple_of(other * hw + j * JC + n * width, width), width)
        landed(hid.at[:, c], h_recv.at[j + n])

    def wrap(v):
        return lax.rem(v + 2 * side, side)

    def piece(c, o, b):
        a = coord[o]
        r = pl.ds(pl.multiple_of(a * br + (b // 2) * qr, qr), qr)
        q = pl.ds(pl.multiple_of(c * CW + o * ow + lax.rem(b, 2) * qc, qc), qc)
        return r, q

    def slab(c, o, a):
        r = pl.ds(pl.multiple_of(a * br, br), br)
        q = pl.ds(pl.multiple_of(c * CW + o * ow, ow), ow)
        return r, q

    def scatter_direct(src, fin, s_fin, sem, pos, dev):
        for d, delta in enumerate((1, -1, 2)):
            send(src.at[wrap(pos + delta)], fin.at[d], s_fin, sem(d), dev[d]).start()

    def scatter_ring(src, fin, s_fin, q_fin, pos, dev):
        for d in (0, 1):
            send(src.at[wrap(pos + 2), d], fin.at[2, d], s_fin, q_fin.at[2, d], dev[d]).start()
        for d in (0, 1):
            send(src.at[wrap(pos + 1 - 2 * d), 1 - d], fin.at[d, 1 - d], s_fin, q_fin.at[d, 1 - d], dev[d]).start()

    def make_term(c):
        t = jnp.dot(hid[:, theirs], pool[c, other], preferred_element_type=F32)
        for o in (0, 1):
            for q in range(side):
                for g in (0, 1):
                    v = t[g * rows + q * br:g * rows + (q + 1) * br, o * ow:(o + 1) * ow]
                    v = v + term[c, o, q, g]
                    term[c, o, q, g] = v
                    termb[c, o, q, g] = v.astype(BF16)
        @pl.when(c < nc - STRAIGHT_1)
        def _():
            for o in (0, 1):
                scatter_ring(termb.at[c, o], f1.at[c, o], s_f1, q_f1.at[c, o], coord[o], nbr[o])

        @pl.when(c >= nc - STRAIGHT_1)
        def _():
            for o in (0, 1):
                scatter_direct(
                    termb.at[c, o], f1.at[c, o], s_f1, lambda d, o=o: q_f1.at[c, o, d, 0], coord[o], nbr[o]
                )

        @pl.when(c + AHEAD < nc)
        def _():
            own_half(c + AHEAD)

    def relay_1(c):
        @pl.when(c < nc - STRAIGHT_1)
        def _():
            for o in (0, 1):
                for d in (0, 1):
                    part = f1.at[c, o, 2, d]
                    landed(part, q_f1.at[c, o, 2, d])
                    part[...] = (part[...].astype(F32) + term[c, o, wrap(coord[o] + 1 - 2 * d), d]).astype(BF16)
                    send(part, f1.at[c, o, d, d], s_f1, q_f1.at[c, o, d, d], nbr[o][d]).start()

    def split_slab(c, o, n):
        for g in (0, 1):
            v = term[c, o, coord[o], g]
            for d in range(n):
                v = v + f1[c, o, d, g].astype(F32)
            for q in range(side):
                w = v[(q // 2) * qr:(q // 2 + 1) * qr, (q % 2) * qc:(q % 2 + 1) * qc]
                red[c, o, q, g] = w
                redb[c, o, q, g] = w.astype(BF16)
        scatter_direct(redb.at[c, o], f2.at[c, o], s_f2, lambda d: q_f2.at[c, o, d], coord[1 - o], nbr[1 - o])

    def reduce_1(c):
        @pl.when(c < nc - STRAIGHT_1)
        def _():
            for o in (0, 1):
                for d in (0, 1):
                    for g in (0, 1):
                        landed(f1.at[c, o, d, g], q_f1.at[c, o, d, g])
                split_slab(c, o, 2)

        @pl.when(c >= nc - STRAIGHT_1)
        def _():
            for o in (0, 1):
                for d in range(3):
                    landed(f1.at[c, o, d], q_f1.at[c, o, d, 0])
                split_slab(c, o, 3)

    def reduce_2(c):
        for o in (0, 1):
            b = coord[1 - o]
            for d in range(3):
                landed(f2.at[c, o, d], q_f2.at[c, o, d])

            def total(g):
                v = red[c, o, b, g] + f2[c, o, 0, g].astype(F32) + f2[c, o, 1, g].astype(F32)
                return (v + f2[c, o, 2, g].astype(F32)).astype(BF16)

            r, q = piece(c, o, b)
            swp[c, o] = total(other)
            send(swp.at[c, o], ybuf.at[h, r, q], s_sw, q_sw.at[c, o], partner).start()
            ybuf[h, r, q] = total(h)

    def gather_1(c):
        for o in (0, 1):
            r, q = piece(c, o, coord[1 - o])
            landed(ybuf.at[other, r, q], q_sw.at[c, o])
            for d in range(3):
                send(ybuf.at[:, r, q], ybuf.at[:, r, q], s_g1, q_g1.at[c, o, d], nbr[1 - o][d]).start()

    def gather_2(c):
        for o in (0, 1):
            for d, delta in enumerate((-1, 1, 2)):
                r, q = piece(c, o, wrap(coord[1 - o] + delta))
                landed(ybuf.at[:, r, q], q_g1.at[c, o, d])
            r, q = slab(c, o, coord[o])
            for d in (0, 1):
                send(ybuf.at[:, r, q], ybuf.at[:, r, q], s_g2, q_g2.at[c, o, d, 0], nbr[o][d]).start()

            @pl.when(c >= nc - STRAIGHT_2)
            def _(o=o, r=r, q=q):
                send(ybuf.at[:, r, q], ybuf.at[:, r, q], s_g2, q_g2.at[c, o, 0, 1], nbr[o][2]).start()

    def forward_2(c):
        for o in (0, 1):
            for d in (0, 1):
                r, q = slab(c, o, wrap(coord[o] - 1 + 2 * d))
                landed(ybuf.at[:, r, q], q_g2.at[c, o, d, 0])

                @pl.when(c < nc - STRAIGHT_2)
                def _(o=o, d=d, r=r, q=q):
                    send(ybuf.at[d, r, q], ybuf.at[d, r, q], s_g2, q_g2.at[c, o, d, 1], nbr[o][d]).start()

    def finish(c):
        @pl.when(c < nc - STRAIGHT_2)
        def _():
            for o in (0, 1):
                r, q = slab(c, o, wrap(coord[o] + 2))
                for d in (0, 1):
                    landed(ybuf.at[d, r, q], q_g2.at[c, o, d, 1])

        @pl.when(c >= nc - STRAIGHT_2)
        def _():
            for o in (0, 1):
                r, q = slab(c, o, wrap(coord[o] + 2))
                landed(ybuf.at[:, r, q], q_g2.at[c, o, 0, 1])

    stages = (make_term, relay_1, reduce_1, reduce_2, gather_1, gather_2, forward_2, finish)

    def tick(t, carry):
        for s, stage in enumerate(stages):
            c = t - s * LAG

            @pl.when((c >= 0) & (c < nc))
            def _(stage=stage, c=c):
                stage(c)

        return carry

    lax.fori_loop(0, nc + (len(stages) - 1) * LAG, tick, 0)

    left_device(ybuf, x_out)
    left_device(hid.at[:, pl.ds(0, hw)], h_out)
    left_device(f1, s_f1)
    left_device(f2, s_f2)
    left_device(swp, s_sw)
    left_device(f2, s_g1)
    left_device(f1, s_g2)


def write_out(y_ref, out_ref, sem):
    rows, cols = y_ref.shape[1:]
    n = sem.shape[1]
    copies = [
        pltpu.make_async_copy(
            y_ref.at[d, pl.ds(i * rows // n, rows // n)],
            out_ref.at[pl.ds(i * rows // n, rows // n), pl.ds(d * cols, cols)],
            sem.at[d, i],
        )
        for d in (0, 1)
        for i in range(n)
    ]
    for cp in copies:
        cp.start()
    for cp in copies:
        cp.wait()


def solution(mesh):
    side = math.isqrt(mesh.shape["tp"])

    def step(x, w_gate, w_up, w_down):
        rows, depth = x.shape
        hw = w_gate.shape[1] // 2
        cols = w_down.shape[1] // 2
        nk, nj, nc = depth // KC, hw // JC, cols // CW
        ow = CW // 2
        br, qr, qc = rows // side, rows // side // 2, ow // 2
        dma = pltpu.SemaphoreType.DMA
        scratch = [
            pltpu.VMEM((2, rows, depth), BF16),
            pltpu.VMEM((nk * nj, 2, KC, JC), BF16),
            pltpu.VMEM((nj, 2, 2, rows, JC), F32),
            pltpu.VMEM((2 * rows, 2 * hw), BF16),
            pltpu.VMEM((nc, 2, side, 2, br, ow), F32),
            pltpu.VMEM((nc, 2, side, 2, br, ow), BF16),
            pltpu.VMEM((nc, 2, 3, 2, br, ow), BF16),
            pltpu.VMEM((nc, 2, side, 2, qr, qc), F32),
            pltpu.VMEM((nc, 2, side, 2, qr, qc), BF16),
            pltpu.VMEM((nc, 2, 3, 2, qr, qc), BF16),
            pltpu.VMEM((nc, 2, qr, qc), BF16),
            dma((nk,)), dma, dma((nk,)), dma((nk * nj, 2)), dma((nc, 2)), dma, dma((nj + 1,)),
            dma, dma, dma, dma, dma,
            dma((nc, 2, 3, 2)), dma((nc, 2, 3)), dma((nc, 2)), dma((nc, 2, 3)), dma((nc, 2, 2, 2)),
        ]
        any_spec = pl.BlockSpec(memory_space=pl.ANY)
        y = pl.pallas_call(
            functools.partial(kernel, side),
            out_shape=jax.ShapeDtypeStruct((2, rows, cols), BF16),
            in_specs=[any_spec] * 4,
            out_specs=pl.BlockSpec(memory_space=pltpu.VMEM),
            scratch_shapes=scratch,
            compiler_params=pltpu.CompilerParams(
                collective_id=0, has_side_effects=True, vmem_limit_bytes=VMEM_LIMIT
            ),
            cost_estimate=pl.CostEstimate(
                flops=6 * rows * depth * 2 * hw, bytes_accessed=6 * depth * hw, transcendentals=2 * rows * hw
            ),
        )(pltpu.with_memory_space_constraint(x, pltpu.HBM), w_gate, w_up, w_down)
        return pl.pallas_call(
            write_out,
            out_shape=jax.ShapeDtypeStruct((rows, 2 * cols), BF16),
            in_specs=[pl.BlockSpec(memory_space=pltpu.VMEM)],
            out_specs=any_spec,
            scratch_shapes=[dma((2, 4))],
            compiler_params=pltpu.CompilerParams(vmem_limit_bytes=1 << 20),
        )(y)

    return jax.shard_map(
        step,
        mesh=mesh,
        in_specs=(P("dp", None), P(None, "tp"), P(None, "tp"), P("tp", None)),
        out_specs=P("dp", None),
        check_vma=False,
    )
```

```python
import functools
import math

import jax
import jax.numpy as jnp
from jax import lax
from jax.experimental import pallas as pl
from jax.experimental.pallas import tpu as pltpu
from jax.sharding import PartitionSpec as P

MESH = pl.DeviceIdType.MESH
F32, BF16 = jnp.float32, jnp.bfloat16

VMEM_LIMIT = 51 << 20
KC = 1024
JC = 512
CW = 512
FIRST = 2
DEPTH = 6
AHEAD = 2
STRAIGHT_1 = 0
STRAIGHT_2 = 3
LAG = 5


def kernel(
    side, x_ref, wg_ref, wu_ref, wd_ref, ybuf,
    xs, pool, acc, hid, term, termb, f1, red, redb, f2, swp,
    x_in, x_out, x_recv, w_in, wd_in, h_out, h_recv,
    s_f1, s_f2, s_sw, s_g1, s_g2, q_f1, q_f2, q_sw, q_g1, q_g2,
):
    rows, depth = x_ref.shape
    hw = wg_ref.shape[1] // 2
    cols = ybuf.shape[2]
    nk, nj, nc = depth // KC, hw // JC, cols // CW
    nblk = nk * nj
    ow = CW // 2
    br, qr, qc = rows // side, rows // side // 2, ow // 2

    dp, tp = lax.axis_index("dp"), lax.axis_index("tp")
    h = lax.rem(dp, 2)
    other = 1 - h
    partner = (dp + 1 - 2 * h, tp)
    cx, cy = tp // side, lax.rem(tp, side)

    def near(axis, d):
        if axis == 0:
            return (dp, lax.rem(cx + d + side, side) * side + cy)
        return (dp, cx * side + lax.rem(cy + d + side, side))

    nbr = [[near(axis, d) for d in (1, -1, 2)] for axis in (0, 1)]
    coord = [cx, cy]

    def send(src, dst, s_sem, r_sem, dev):
        return pltpu.make_async_remote_copy(
            src_ref=src, dst_ref=dst, send_sem=s_sem, recv_sem=r_sem, device_id=dev, device_id_type=MESH
        )

    def landed(dst, r_sem):
        pltpu.make_async_remote_copy(
            src_ref=dst, dst_ref=dst, send_sem=s_sw, recv_sem=r_sem, device_id=partner, device_id_type=MESH
        ).wait_recv()

    def left_device(ref, s_sem):
        pltpu.make_async_remote_copy(
            src_ref=ref, dst_ref=ref, send_sem=s_sem, recv_sem=s_sem, device_id=partner, device_id_type=MESH
        ).wait_send()

    def x_piece(k):
        c = pl.ds(k * KC, KC)
        return pltpu.make_async_copy(x_ref.at[:, c], xs.at[h, :, c], x_in.at[k])

    def w_block(i):
        j, k = i // nk, lax.rem(i, nk)
        r = pl.ds(pl.multiple_of(k * KC, KC), KC)
        c = pl.ds(pl.multiple_of(h * hw + j * JC, JC), JC)
        return [
            pltpu.make_async_copy(ref.at[r, c], pool.at[i, m], w_in.at[i, m]) for m, ref in enumerate((wg_ref, wu_ref))
        ]

    def wd_block(c):
        cc = pl.ds(pl.multiple_of(h * cols + c * CW, CW), CW)
        return [
            pltpu.make_async_copy(wd_ref.at[pl.ds(m * hw, hw), cc], pool.at[c, m], wd_in.at[c, m]) for m in (0, 1)
        ]

    def wait_all(copies):
        for cp in copies:
            cp.wait()

    def start_all(copies):
        for cp in copies:
            cp.start()

    barrier = pltpu.get_barrier_semaphore()
    for dev in (partner, *nbr[0], *nbr[1]):
        pl.semaphore_signal(barrier, inc=1, device_id=dev, device_id_type=MESH)

    for k in range(nk):
        x_piece(k).start()
    for i in range(FIRST):
        start_all(w_block(i))
    acc[...] = jnp.zeros_like(acc)

    def chunk_of_x(k):
        return pl.ds(pl.multiple_of(k * KC, KC), KC)

    def following(i):
        @pl.when(i < nblk)
        def _():
            start_all(w_block(i))

        @pl.when(i >= nblk)
        def _():
            start_all(wd_block(i - nblk))

    def all_rows(j, k):
        wait_all(w_block(j * nk + k))
        following(j * nk + k + DEPTH)
        lhs = xs[:, :, chunk_of_x(k)].reshape(2 * rows, KC)
        for m in (0, 1):
            acc[j, m] += jnp.dot(lhs, pool[j * nk + k, m], preferred_element_type=F32).reshape(2, rows, JC)

    def send_hidden(j, n, width):
        c = pl.ds(pl.multiple_of(h * hw + j * JC + n * width, width), width)
        send(hid.at[:, c], hid.at[:, c], h_out, h_recv.at[j + n], partner).start()

    pl.semaphore_wait(barrier, 7)
    for k in range(nk):
        x_piece(k).wait()
        c = pl.ds(k * KC, KC)
        send(xs.at[h, :, c], xs.at[h, :, c], x_out, x_recv.at[k], partner).start()
    for i in range(FIRST, DEPTH):
        start_all(w_block(i))

    def first_half(k, carry):
        landed(xs.at[other, :, chunk_of_x(k)], x_recv.at[k])
        all_rows(0, k)
        return carry

    lax.fori_loop(0, nk, first_half, 0, unroll=2)

    def with_act(t, carry):
        all_rows(1, t)
        hc = pl.ds(pl.multiple_of(h * hw, JC), JC)
        hid[pl.ds(pl.multiple_of(t * rows, rows), rows), hc] = (
            jax.nn.silu(acc[0, 0, t]) * acc[0, 1, t]
        ).astype(BF16)
        return carry

    lax.fori_loop(0, 2, with_act, 0)
    send_hidden(0, 0, JC)

    def second_half(k, carry):
        all_rows(1, k)
        return carry

    lax.fori_loop(2, nk - 1, second_half, 0, unroll=True)
    k = nk - 1
    wait_all(w_block(nk + k))
    following(nk + k + DEPTH)
    lhs = xs[:, :, chunk_of_x(k)].reshape(2 * rows, KC)
    half = JC // 2
    for n in (0, 1):
        cc = slice(n * half, (n + 1) * half)
        g, u = (
            acc[1, m, :, :, cc].reshape(2 * rows, half)
            + jnp.dot(lhs, pool[nk + k, m, :, cc], preferred_element_type=F32)
            for m in (0, 1)
        )
        hid[:, pl.ds(pl.multiple_of(h * hw + JC + n * half, half), half)] = (jax.nn.silu(g) * u).astype(BF16)
        send_hidden(1, n, half)

    mine = pl.ds(pl.multiple_of(h * hw, hw), hw)
    theirs = pl.ds(pl.multiple_of(other * hw, hw), hw)

    def own_half(c):
        wait_all(wd_block(c))

        @pl.when(c + DEPTH < nc)
        def _():
            start_all(wd_block(c + DEPTH))

        t = jnp.dot(hid[:, mine], pool[c, h], preferred_element_type=F32)
        for o in (0, 1):
            for q in range(side):
                for g in (0, 1):
                    term[c, o, q, g] = t[g * rows + q * br:g * rows + (q + 1) * br, o * ow:(o + 1) * ow]

    def ahead(c, carry):
        own_half(c)
        return carry

    lax.fori_loop(0, AHEAD, ahead, 0)
    for j, n, width in ((0, 0, JC), (1, 0, half), (1, 1, half)):
        c = pl.ds(pl.multiple_of(other * hw + j * JC + n * width, width), width)
        landed(hid.at[:, c], h_recv.at[j + n])

    def wrap(v):
        return lax.rem(v + 2 * side, side)

    def piece(c, o, b):
        a = coord[o]
        r = pl.ds(pl.multiple_of(a * br + (b // 2) * qr, qr), qr)
        q = pl.ds(pl.multiple_of(c * CW + o * ow + lax.rem(b, 2) * qc, qc), qc)
        return r, q

    def slab(c, o, a):
        r = pl.ds(pl.multiple_of(a * br, br), br)
        q = pl.ds(pl.multiple_of(c * CW + o * ow, ow), ow)
        return r, q

    def scatter_direct(src, fin, s_fin, sem, pos, dev):
        for d, delta in enumerate((1, -1, 2)):
            send(src.at[wrap(pos + delta)], fin.at[d], s_fin, sem(d), dev[d]).start()

    def scatter_ring(src, fin, s_fin, q_fin, pos, dev):
        for d in (0, 1):
            send(src.at[wrap(pos + 2), d], fin.at[2, d], s_fin, q_fin.at[2, d], dev[d]).start()
        for d in (0, 1):
            send(src.at[wrap(pos + 1 - 2 * d), 1 - d], fin.at[d, 1 - d], s_fin, q_fin.at[d, 1 - d], dev[d]).start()

    def make_term(c):
        t = jnp.dot(hid[:, theirs], pool[c, other], preferred_element_type=F32)
        for o in (0, 1):
            for q in range(side):
                for g in (0, 1):
                    v = t[g * rows + q * br:g * rows + (q + 1) * br, o * ow:(o + 1) * ow]
                    v = v + term[c, o, q, g]
                    term[c, o, q, g] = v
                    termb[c, o, q, g] = v.astype(BF16)
        @pl.when(c < nc - STRAIGHT_1)
        def _():
            for o in (0, 1):
                scatter_ring(termb.at[c, o], f1.at[c, o], s_f1, q_f1.at[c, o], coord[o], nbr[o])

        @pl.when(c >= nc - STRAIGHT_1)
        def _():
            for o in (0, 1):
                scatter_direct(
                    termb.at[c, o], f1.at[c, o], s_f1, lambda d, o=o: q_f1.at[c, o, d, 0], coord[o], nbr[o]
                )

        @pl.when(c + AHEAD < nc)
        def _():
            own_half(c + AHEAD)

    def relay_1(c):
        @pl.when(c < nc - STRAIGHT_1)
        def _():
            for o in (0, 1):
                for d in (0, 1):
                    part = f1.at[c, o, 2, d]
                    landed(part, q_f1.at[c, o, 2, d])
                    part[...] = (part[...].astype(F32) + term[c, o, wrap(coord[o] + 1 - 2 * d), d]).astype(BF16)
                    send(part, f1.at[c, o, d, d], s_f1, q_f1.at[c, o, d, d], nbr[o][d]).start()

    def split_slab(c, o, n):
        for g in (0, 1):
            v = term[c, o, coord[o], g]
            for d in range(n):
                v = v + f1[c, o, d, g].astype(F32)
            for q in range(side):
                w = v[(q // 2) * qr:(q // 2 + 1) * qr, (q % 2) * qc:(q % 2 + 1) * qc]
                red[c, o, q, g] = w
                redb[c, o, q, g] = w.astype(BF16)
        scatter_direct(redb.at[c, o], f2.at[c, o], s_f2, lambda d: q_f2.at[c, o, d], coord[1 - o], nbr[1 - o])

    def reduce_1(c):
        @pl.when(c < nc - STRAIGHT_1)
        def _():
            for o in (0, 1):
                for d in (0, 1):
                    for g in (0, 1):
                        landed(f1.at[c, o, d, g], q_f1.at[c, o, d, g])
                split_slab(c, o, 2)

        @pl.when(c >= nc - STRAIGHT_1)
        def _():
            for o in (0, 1):
                for d in range(3):
                    landed(f1.at[c, o, d], q_f1.at[c, o, d, 0])
                split_slab(c, o, 3)

    def reduce_2(c):
        for o in (0, 1):
            b = coord[1 - o]
            for d in range(3):
                landed(f2.at[c, o, d], q_f2.at[c, o, d])

            def total(g):
                v = red[c, o, b, g] + f2[c, o, 0, g].astype(F32) + f2[c, o, 1, g].astype(F32)
                return (v + f2[c, o, 2, g].astype(F32)).astype(BF16)

            r, q = piece(c, o, b)
            swp[c, o] = total(other)
            send(swp.at[c, o], ybuf.at[h, r, q], s_sw, q_sw.at[c, o], partner).start()
            ybuf[h, r, q] = total(h)

    def gather_1(c):
        for o in (0, 1):
            r, q = piece(c, o, coord[1 - o])
            landed(ybuf.at[other, r, q], q_sw.at[c, o])
            for d in range(3):
                send(ybuf.at[:, r, q], ybuf.at[:, r, q], s_g1, q_g1.at[c, o, d], nbr[1 - o][d]).start()

    def gather_2(c):
        for o in (0, 1):
            for d, delta in enumerate((-1, 1, 2)):
                r, q = piece(c, o, wrap(coord[1 - o] + delta))
                landed(ybuf.at[:, r, q], q_g1.at[c, o, d])
            r, q = slab(c, o, coord[o])
            for d in (0, 1):
                send(ybuf.at[:, r, q], ybuf.at[:, r, q], s_g2, q_g2.at[c, o, d, 0], nbr[o][d]).start()

            @pl.when(c >= nc - STRAIGHT_2)
            def _(o=o, r=r, q=q):
                send(ybuf.at[:, r, q], ybuf.at[:, r, q], s_g2, q_g2.at[c, o, 0, 1], nbr[o][2]).start()

    def forward_2(c):
        for o in (0, 1):
            for d in (0, 1):
                r, q = slab(c, o, wrap(coord[o] - 1 + 2 * d))
                landed(ybuf.at[:, r, q], q_g2.at[c, o, d, 0])

                @pl.when(c < nc - STRAIGHT_2)
                def _(o=o, d=d, r=r, q=q):
                    send(ybuf.at[d, r, q], ybuf.at[d, r, q], s_g2, q_g2.at[c, o, d, 1], nbr[o][d]).start()

    def finish(c):
        @pl.when(c < nc - STRAIGHT_2)
        def _():
            for o in (0, 1):
                r, q = slab(c, o, wrap(coord[o] + 2))
                for d in (0, 1):
                    landed(ybuf.at[d, r, q], q_g2.at[c, o, d, 1])

        @pl.when(c >= nc - STRAIGHT_2)
        def _():
            for o in (0, 1):
                r, q = slab(c, o, wrap(coord[o] + 2))
                landed(ybuf.at[:, r, q], q_g2.at[c, o, 0, 1])

    stages = (make_term, relay_1, reduce_1, reduce_2, gather_1, gather_2, forward_2, finish)

    def tick(t, carry):
        for s, stage in enumerate(stages):
            c = t - s * LAG

            @pl.when((c >= 0) & (c < nc))
            def _(stage=stage, c=c):
                stage(c)

        return carry

    lax.fori_loop(0, nc + (len(stages) - 1) * LAG, tick, 0)

    left_device(ybuf, x_out)
    left_device(hid.at[:, pl.ds(0, hw)], h_out)
    left_device(f1, s_f1)
    left_device(f2, s_f2)
    left_device(swp, s_sw)
    left_device(f2, s_g1)
    left_device(f1, s_g2)


def write_out(y_ref, out_ref, sem):
    rows, cols = y_ref.shape[1:]
    n = sem.shape[1]
    copies = [
        pltpu.make_async_copy(
            y_ref.at[d, pl.ds(i * rows // n, rows // n)],
            out_ref.at[pl.ds(i * rows // n, rows // n), pl.ds(d * cols, cols)],
            sem.at[d, i],
        )
        for d in (0, 1)
        for i in range(n)
    ]
    for cp in copies:
        cp.start()
    for cp in copies:
        cp.wait()


def solution(mesh):
    side = math.isqrt(mesh.shape["tp"])

    def step(x, w_gate, w_up, w_down):
        rows, depth = x.shape
        hw = w_gate.shape[1] // 2
        cols = w_down.shape[1] // 2
        nk, nj, nc = depth // KC, hw // JC, cols // CW
        ow = CW // 2
        br, qr, qc = rows // side, rows // side // 2, ow // 2
        dma = pltpu.SemaphoreType.DMA
        scratch = [
            pltpu.VMEM((2, rows, depth), BF16),
            pltpu.VMEM((nk * nj, 2, KC, JC), BF16),
            pltpu.VMEM((nj, 2, 2, rows, JC), F32),
            pltpu.VMEM((2 * rows, 2 * hw), BF16),
            pltpu.VMEM((nc, 2, side, 2, br, ow), F32),
            pltpu.VMEM((nc, 2, side, 2, br, ow), BF16),
            pltpu.VMEM((nc, 2, 3, 2, br, ow), BF16),
            pltpu.VMEM((nc, 2, side, 2, qr, qc), F32),
            pltpu.VMEM((nc, 2, side, 2, qr, qc), BF16),
            pltpu.VMEM((nc, 2, 3, 2, qr, qc), BF16),
            pltpu.VMEM((nc, 2, qr, qc), BF16),
            dma((nk,)), dma, dma((nk,)), dma((nk * nj, 2)), dma((nc, 2)), dma, dma((nj + 1,)),
            dma, dma, dma, dma, dma,
            dma((nc, 2, 3, 2)), dma((nc, 2, 3)), dma((nc, 2)), dma((nc, 2, 3)), dma((nc, 2, 2, 2)),
        ]
        any_spec = pl.BlockSpec(memory_space=pl.ANY)
        y = pl.pallas_call(
            functools.partial(kernel, side),
            out_shape=jax.ShapeDtypeStruct((2, rows, cols), BF16),
            in_specs=[any_spec] * 4,
            out_specs=pl.BlockSpec(memory_space=pltpu.VMEM),
            scratch_shapes=scratch,
            compiler_params=pltpu.CompilerParams(
                collective_id=0, has_side_effects=True, vmem_limit_bytes=VMEM_LIMIT
            ),
            cost_estimate=pl.CostEstimate(
                flops=6 * rows * depth * 2 * hw, bytes_accessed=6 * depth * hw, transcendentals=2 * rows * hw
            ),
        )(pltpu.with_memory_space_constraint(x, pltpu.HBM), w_gate, w_up, w_down)
        return pl.pallas_call(
            write_out,
            out_shape=jax.ShapeDtypeStruct((rows, 2 * cols), BF16),
            in_specs=[pl.BlockSpec(memory_space=pltpu.VMEM)],
            out_specs=any_spec,
            scratch_shapes=[dma((2, 4))],
            compiler_params=pltpu.CompilerParams(vmem_limit_bytes=1 << 20),
        )(y)

    return jax.shard_map(
        step,
        mesh=mesh,
        in_specs=(P("dp", None), P(None, "tp"), P(None, "tp"), P("tp", None)),
        out_specs=P("dp", None),
        check_vma=False,
    )
```
